32 devices in a mesh: row: 2 (over y), col: 4 (over z), depth: 4 (over x, core).
Axes of the slice: x: 2, y: 2, z: 4, core: 2. Of those that a mesh axis runs over, the one named last changes fastest.
Arguments:
- state_matrix: float32 [6144, 6144], P('row', 'col'), as said below
- gram_factor: float32 [6144, 256], P(('col', 'depth'), 'row'), as said below
Outputs:
- squared: float32 [6144, 6144], P('row', ('col', 'depth'))
- appended: float32 [6144, 256], P(('row', 'col', 'depth'))
- norm_ratio: float32 [256], replicated
Inputs may be any that keep to these rules, and one draw needn't show every extreme that they name: `gram_factor`: entries whose scale grows up to about ninefold along the rows; the columns differ in scale by up to tenfold. `state_matrix`: A real matrix with entries of order one on the diagonal and smaller ones elsewhere.
All inputs are finite; a program needn't handle non-finite values.
Results may differ from the reference program's by a relative error of at most 0.000073.
Values sent between devices are 32-bit elements; how exact they have to be, the bound alone decides.
A program may use at most 128 MiB of HBM per device.

```python
import math
import jax
import jax.numpy as jnp
from jax import lax

ORDER = 6144
RANK = 256


def draw_state_matrix(key, part):
    first, second, third = jax.random.split(jax.random.fold_in(key, 11), 3)
    noise = jax.random.normal(first, (ORDER, ORDER), jnp.float32)
    magnitude = jax.random.uniform(second, (ORDER,), jnp.float32, 0.1, 0.9)
    signs = jnp.where(jax.random.uniform(third, (ORDER,), jnp.float32) < 0.5, -1.0, 1.0)
    return noise * (0.6 / math.sqrt(ORDER)) + jnp.diag(signs * magnitude)


def draw_gram_factor(key, part):
    first, second, third = jax.random.split(jax.random.fold_in(key, 23), 3)
    positions = jnp.arange(ORDER, dtype=jnp.float32) / ORDER
    row_scale = jnp.exp(math.log(3.0) * positions + jax.random.uniform(second, (ORDER,), jnp.float32, 0.0, math.log(3.0)))
    col_scale = jnp.exp(jax.random.uniform(third, (RANK,), jnp.float32, math.log(0.3), math.log(3.0)))
    noise = jax.random.normal(first, (ORDER, RANK), jnp.float32)
    return noise * row_scale[:, None] * col_scale[None, :]


def setup_inputs(seed: int = 0) -> dict:
    streams_of = jax.random.split(jax.random.key(seed), 3)
    state_matrix = draw_state_matrix(jax.random.fold_in(streams_of[2], 71), 0)
    gram_factor = draw_gram_factor(jax.random.fold_in(streams_of[2], 71), 0)
    return {"state_matrix": state_matrix, "gram_factor": gram_factor}


def reference(state_matrix, gram_factor):
    squared = jnp.dot(state_matrix, state_matrix, preferred_element_type=jnp.float32, precision=lax.Precision.HIGHEST)
    appended = jnp.dot(state_matrix, gram_factor, preferred_element_type=jnp.float32, precision=lax.Precision.HIGHEST)
    new_sq = lax.optimization_barrier(jnp.sum(appended * appended, axis=0))
    old_sq = lax.optimization_barrier(jnp.sum(gram_factor * gram_factor, axis=0))
    norm_ratio = jnp.sqrt(new_sq) / jnp.sqrt(old_sq + 1e-06)
    return (squared, appended, norm_ratio)
```

```python
import jax
import jax.numpy as jnp
from jax import lax
from jax.sharding import PartitionSpec as P


def product(left, right):
    return jnp.dot(left, right, preferred_element_type=jnp.float32, precision=lax.Precision.HIGH)


def halving_order(count):
    order = [0]
    step = 1
    while step < count:
        order = [2 * j for j in order] + [2 * j + 1 for j in order]
        step *= 2
    return order


def exchange(value, bit, count):
    return lax.ppermute(value, "depth", [(d, d ^ bit) for d in range(count)])


def body(state_matrix, gram_factor):
    row_count = lax.axis_size("row")
    col_count = lax.axis_size("col")
    depth_count = lax.axis_size("depth")
    row_index = lax.axis_index("row")
    col_index = lax.axis_index("col")
    depth_index = lax.axis_index("depth")
    block_rows, block_cols = state_matrix.shape
    slab = block_cols // depth_count
    blocks_per_row = block_rows // block_cols
    order = halving_order(depth_count)

    own_columns = lax.dynamic_slice_in_dim(state_matrix, depth_index * slab, slab, 1)
    edges = [block_rows * part // 16 for part in (0, 7, 13, 16)]
    lefts = [
        lax.all_gather(own_columns[low:high], "col", axis=1, tiled=True) for low, high in zip(edges, edges[1:])
    ]

    stacked = state_matrix.reshape(blocks_per_row, block_cols, block_cols)
    own_rows = lax.dynamic_slice_in_dim(stacked, depth_index * slab, slab, 1).reshape(
        blocks_per_row * slab, block_cols
    )
    own_rows = jnp.concatenate(
        [lax.dynamic_slice_in_dim(own_rows, (depth_index ^ j) * slab, slab, 1) for j in order], axis=1
    )

    def row_gather(value):
        pieces = [value]
        for s in range(1, row_count):
            pieces.append(lax.ppermute(value, "row", [(r, (r + s) % row_count) for r in range(row_count)]))
        ordered = []
        for r in range(row_count):
            piece = pieces[0]
            for s in range(1, row_count):
                piece = jnp.where(lax.rem(row_index + (row_count - r), row_count) == s, pieces[s], piece)
            ordered.append(piece)
        return ordered

    factor_block = jnp.concatenate(row_gather(gram_factor), axis=1)
    column_block = jnp.concatenate(row_gather(own_rows), axis=0)

    terms = product(own_columns, factor_block)
    piece_rows = block_rows // (col_count * depth_count)
    terms = terms.reshape(col_count, depth_count, piece_rows, terms.shape[1])
    held = jnp.concatenate(
        [lax.dynamic_slice_in_dim(terms, depth_index ^ j, 1, 1) for j in order], axis=1
    )
    bit, width = 1, depth_count
    while width > 1:
        width //= 2
        held = held[:, :width] + exchange(held[:, width:], bit, depth_count)
        bit *= 2
    held = held[:, 0]
    new_rows = lax.dynamic_index_in_dim(held, col_index, 0, keepdims=False)
    for s in range(1, col_count):
        part = lax.dynamic_index_in_dim(held, lax.rem(col_index + s, col_count), 0, keepdims=False)
        new_rows = new_rows + lax.ppermute(part, "col", [(c, (c + s) % col_count) for c in range(col_count)])
    new_sq = jnp.sum(new_rows * new_rows, axis=0)
    old_sq = jnp.sum(factor_block * factor_block, axis=0) * (1.0 / row_count)
    totals_new, totals_old = lax.psum((new_sq, old_sq), ("row", "col", "depth"))
    norm_ratio = jnp.sqrt(totals_new) / jnp.sqrt(totals_old + 1e-06)

    half = block_cols // 2
    outs = []
    for left in lefts:
        if outs:
            left, outs[-1], norm_ratio = lax.optimization_barrier((left, outs[-1], norm_ratio))
        if depth_count == 1:
            outs.append(product(left, column_block))
            continue
        sent = exchange(product(left, column_block[:, half:]), 1, depth_count)
        total = product(left, column_block[:, :half]) + sent
        bit, width = 2, half
        while width > slab:
            width //= 2
            total = total[:, :width] + exchange(total[:, width:], bit, depth_count)
            bit *= 2
        outs.append(total)
    squared = jnp.concatenate(outs, axis=0)
    return (squared, new_rows, norm_ratio)


def solution(mesh):
    in_specs = (P("row", "col"), P(("col", "depth"), "row"))
    out_specs = (P("row", ("col", "depth")), P(("row", "col", "depth"), None), P())
    return jax.shard_map(body, mesh=mesh, in_specs=in_specs, out_specs=out_specs, check_vma=False)
```
